32 devices in a mesh: seq: 8 (over y, x, core), head: 4 (over z).
Axes of the slice: x: 2, y: 2, z: 4, core: 2. Of those that a mesh axis runs over, the one named last changes fastest.
Arguments:
- mid: bfloat16 [2048, 3072], P('seq'), may hold values from -20 to 20
- second_in: bfloat16 [2048, 3072], P('seq'), may hold values from -20 to 20
- cotangent: bfloat16 [2048, 3072], P('seq'), may hold values from -6 to 6
- w_key: bfloat16 [3072, 1024], P(None, 'head'), may hold values from -0.109375 to 0.109375
- w_value: bfloat16 [3072, 1024], P(None, 'head'), may hold values from -0.109375 to 0.109375
- w_query: bfloat16 [2, 3072, 3072], P(None, None, 'head'), may hold values from -0.109375 to 0.109375
- w_out: bfloat16 [2, 3072, 3072], P(None, 'head'), may hold values from -0.109375 to 0.109375
- w_ret_out: bfloat16 [3072, 3072], P('head'), may hold values from -0.109375 to 0.109375
- ret_query: bfloat16 [2048, 3072], P('seq', 'head'), may hold values from -6 to 6
- ret_key: bfloat16 [2048, 3072], P('seq', 'head'), may hold values from -3 to 3
- ret_value: bfloat16 [2048, 3072], P('seq', 'head'), may hold values from -6 to 6
- gate: float32 [24, 2048], P('head', 'seq'), may hold values from 0 to 6
- decay_exp: int32 [24], P('head'), may hold values from 0 to 256
- mask_start: int32 [16], P('seq'), may hold values from 0 to 1920, as said below
Outputs:
- grad_mid: bfloat16 [2048, 3072], P('seq')
- grad_ret_query: bfloat16 [2048, 3072], P('seq', 'head')
- grad_ret_key: bfloat16 [2048, 3072], P('seq', 'head')
- grad_ret_value: bfloat16 [2048, 3072], P('seq', 'head')
- grad_w_key: float32 [3072, 1024], P(None, 'head')
- grad_w_value: float32 [3072, 1024], P(None, 'head')
The draws below stay inside these ranges and needn't reach their ends.
Inputs may be any that keep to these rules, and one draw needn't show every extreme that they name: `mask_start`: the entry of each block of 128 queries is at most the position of that block's first query.
All inputs are finite; a program needn't handle non-finite values.
Results may differ from the reference program's by a relative error of at most 0.025.
The reference program's roundings to bfloat16 on the way count: a program that leaves them out, or rounds other values in their place, can miss the bound.
Values may be sent and summed in bfloat16 or wider, within the bound.
No kernel may reach another device: no remote copies, remote signals or barrier semaphores. Data moves between devices by JAX's collectives and lax.ppermute only.
A program may use at most 192 MiB of HBM per device.

```python
import math
import jax
import jax.numpy as jnp
from jax import lax

D = 3072
H = 24
KVH = 8
HR = 24
E = 128
LAYERS = 2
BLK = 128
RC = 128
TOK_DEV = 256
TOKENS = 2048


def rows_with_peaks(key):
    values = jnp.clip(jax.random.normal(key, (TOKENS, D), jnp.float32), -5.0, 5.0)
    return values.astype(jnp.bfloat16)


def draw_mid(key, part):
    return rows_with_peaks(key)


def draw_second_in(key, part):
    return rows_with_peaks(jax.random.fold_in(key, 11))


def draw_gate(key, part):
    chooser, rough_key, block_key = jax.random.split(key, 3)
    portion = 0.5
    lasting = jax.random.uniform(chooser, (HR, 1), jnp.float32) < portion
    rough = jax.random.uniform(rough_key, (HR, TOKENS), jnp.float32, 0.5, 2.0)
    blocks = jax.random.uniform(block_key, (HR, TOKENS // TOK_DEV), jnp.float32, 0.5, 2.0)
    rough = rough * jnp.repeat(blocks, TOK_DEV, axis=1)
    factor = jnp.where(lasting, 0.5 / TOKENS, 1.5)
    return (factor * rough).astype(jnp.float32)


def draw_mask_start(key, part):
    blocks = TOKENS // BLK
    firsts = jnp.arange(blocks, dtype=jnp.int32) * BLK
    drawn = jax.random.randint(key, (blocks,), 0, firsts + 1, dtype=jnp.int32)
    last_block = jnp.arange(blocks, dtype=jnp.int32) == blocks - 1
    return jnp.where(last_block, firsts, drawn).astype(jnp.int32)


def with_ends(result, stream_key, least, top_value):
    longest = result.shape.index(max(result.shape))
    spots = []
    for shift in (0, 1):
        where = [jax.random.randint(jax.random.fold_in(stream_key, axis), (), 0, length) for axis, length in enumerate(result.shape)]
        where[longest] = (where[longest] + shift) % result.shape[longest]
        spots.append(tuple(where))
    return result.at[spots[0]].set(least).at[spots[1]].set(top_value)


def steps_of(rng, dims, cuts, smallest, high):
    loudness = 1.0
    for position, parts in cuts:
        steps = jax.random.uniform(jax.random.fold_in(jax.random.fold_in(rng, 6), position), (parts,), jnp.float32, smallest / len(cuts), high / len(cuts))
        loudness = loudness * jnp.repeat(jnp.exp(steps), dims[position] // parts).reshape((-1,) + (1,) * (len(dims) - 1 - position))
    return loudness


def gaussian(rng, shape, spread, bound, shards=(), kind=jnp.bfloat16):
    factor_of = steps_of(rng, shape, shards, -0.22, 0.18) if shards else 1.0
    result = jax.random.normal(rng, shape, jnp.float32) * spread * factor_of
    return jnp.minimum(jnp.maximum(result, -bound), bound).astype(kind)


def setup_inputs(seed: int = 0) -> dict:
    streams_of = jax.random.split(jax.random.key(seed), 15)
    return {
        "mid": draw_mid(jax.random.fold_in(streams_of[14], 71), 0),
        "second_in": draw_second_in(jax.random.fold_in(streams_of[14], 71), 0),
        "cotangent": gaussian(streams_of[2], (TOKENS, D), 1.0, 6.0, ((0, 8),)),
        "w_key": gaussian(streams_of[3], (D, KVH * E), D ** -0.5, 0.109375, ((1, 4),)),
        "w_value": gaussian(streams_of[4], (D, KVH * E), D ** -0.5, 0.109375, ((1, 4),)),
        "w_query": gaussian(streams_of[5], (LAYERS, D, H * E), D ** -0.5, 0.109375, ((2, 4),)),
        "w_out": gaussian(streams_of[6], (LAYERS, H * E, D), (H * E) ** -0.5, 0.109375, ((1, 4),)),
        "w_ret_out": gaussian(streams_of[7], (HR * E, D), (HR * E) ** -0.5, 0.109375, ((0, 4),)),
        "ret_query": gaussian(streams_of[8], (TOKENS, HR * E), 1.0, 6.0, ((0, 8), (1, 4))),
        "ret_key": gaussian(streams_of[9], (TOKENS, HR * E), 0.5, 3.0, ((0, 8), (1, 4))),
        "ret_value": gaussian(streams_of[10], (TOKENS, HR * E), 1.0, 6.0, ((0, 8), (1, 4))),
        "gate": draw_gate(jax.random.fold_in(streams_of[14], 71), 0),
        "decay_exp": with_ends(jax.random.randint(streams_of[12], (HR,), 0, 257), jax.random.fold_in(streams_of[12], 1), 0, 256).astype(jnp.int32),
        "mask_start": draw_mask_start(jax.random.fold_in(streams_of[14], 71), 0),
    }


def contract_last(left, right):
    return lax.dot_general(left, right, (((1,), (1,)), ((), ())), preferred_element_type=jnp.float32)

def round_trip(value):
    return lax.optimization_barrier(value.astype(jnp.bfloat16)).astype(jnp.float32)

def attend_back(layer_in, w_query_l, w_out_l, upstream, keys, values, visible):
    length = layer_in.shape[0]
    kv_heads = keys.shape[1] // E
    factor = 1.0 / math.sqrt(E)
    queries = jnp.dot(layer_in, w_query_l, preferred_element_type=jnp.float32).astype(jnp.bfloat16)
    group = queries.shape[1] // keys.shape[1]
    grad_out = contract_last(upstream, w_out_l).astype(jnp.bfloat16)
    query_heads = queries.reshape(length, kv_heads, group, E).transpose(1, 2, 0, 3)
    grad_heads = grad_out.reshape(length, kv_heads, group, E).transpose(1, 2, 0, 3)
    key_heads = keys.reshape(length, kv_heads, E).transpose(1, 0, 2)
    value_heads = values.reshape(length, kv_heads, E).transpose(1, 0, 2)

    def one_group(items):
        query_now = items[0].astype(jnp.float32)
        grad_now = items[1].astype(jnp.float32)
        key_now = items[2].astype(jnp.float32)
        value_now = items[3].astype(jnp.float32)
        scores = jnp.einsum('gte,se->gts', query_now, key_now) * factor
        scores = jnp.where(visible, scores, -jnp.inf)
        top = lax.optimization_barrier(jnp.max(scores, axis=-1, keepdims=True))
        raised = jnp.exp(scores - top)
        probs = raised / lax.optimization_barrier(jnp.sum(raised, axis=-1, keepdims=True))
        rounded = round_trip(probs)
        outputs = round_trip(jnp.einsum('gts,se->gte', rounded, value_now))
        delta = lax.optimization_barrier(jnp.sum(grad_now * outputs, axis=-1, keepdims=True))
        dprobs = jnp.einsum('gte,se->gts', grad_now, value_now)
        dscores = round_trip(probs * (dprobs - delta) * factor)
        query_grad = jnp.einsum('gts,se->gte', dscores, key_now).astype(jnp.bfloat16)
        key_part = jnp.einsum('gts,gte->se', dscores, query_now)
        value_part = jnp.einsum('gts,gte->se', rounded, grad_now)
        return (query_grad, key_part, value_part)
    query_grads, key_parts, value_parts = lax.map(one_group, (query_heads, grad_heads, key_heads, value_heads))
    query_grad = query_grads.transpose(2, 0, 1, 3).reshape(length, -1)
    key_part = key_parts.transpose(1, 0, 2).reshape(length, -1)
    value_part = value_parts.transpose(1, 0, 2).reshape(length, -1)
    return (contract_last(query_grad, w_query_l), key_part, value_part)

def retention_states(ret_key, ret_value, gate, decay_exp):
    length, width = ret_key.shape
    heads = gate.shape[0]
    size = width // heads
    count = length // RC
    key_blocks = ret_key.reshape(count, RC, heads, size).astype(jnp.float32)
    value_blocks = ret_value.reshape(count, RC, heads, size).astype(jnp.float32)
    rate = jnp.exp2(-decay_exp.astype(jnp.float32) / 64.0)
    accum = jnp.cumsum((-rate[:, None] * gate).reshape(heads, count, RC), axis=2)
    ends = accum[:, :, -1]
    shrink = jnp.transpose(jnp.exp(ends[:, :, None] - accum), (1, 2, 0))[..., None]
    own_state = jnp.einsum('csha,cshb->hcab', round_trip(shrink * key_blocks), value_blocks)
    return (accum, ends, shrink, own_state)

def grad_states(ret_query, grad_o, accum):
    heads, count, block = accum.shape
    size = ret_query.shape[1] // heads
    query_blocks = ret_query.reshape(count, block, heads, size).astype(jnp.float32)
    grad_blocks = grad_o.reshape(count, block, heads, size).astype(jnp.float32)
    grow = jnp.transpose(jnp.exp(accum), (1, 2, 0))[..., None]
    own_grad = jnp.einsum('ctha,cthb->hcab', round_trip(grow * query_blocks), grad_blocks) / E
    return (grow, own_grad)

def retention_grads(ret_query, ret_key, ret_value, grad_o, accum, shrink, grow, entering, after):
    length, width = ret_query.shape
    heads, count, block = accum.shape
    size = width // heads
    shape4 = (count, block, heads, size)
    query_blocks = ret_query.reshape(shape4).astype(jnp.float32)
    key_blocks = ret_key.reshape(shape4).astype(jnp.float32)
    value_blocks = ret_value.reshape(shape4).astype(jnp.float32)
    grad_blocks = grad_o.reshape(shape4).astype(jnp.float32)
    lower = jnp.arange(block)[:, None] >= jnp.arange(block)[None, :]
    diff = accum[:, :, :, None] - accum[:, :, None, :]
    weights = jnp.where(lower, jnp.exp(jnp.where(lower, diff, 0.0)), 0.0)
    first = round_trip(weights * jnp.einsum('ctha,csha->hcts', grad_blocks, value_blocks))
    second = round_trip(weights * jnp.einsum('ctha,csha->hcts', query_blocks, key_blocks))
    inner_query = jnp.einsum('hcts,csha->ctha', first, key_blocks)
    inner_key = jnp.einsum('hcts,ctha->csha', first, query_blocks)
    inner_value = jnp.einsum('hcts,ctha->csha', second, grad_blocks)
    highest = lax.Precision.HIGHEST
    carried_query = jnp.einsum('cthb,hcab->ctha', grad_blocks, entering, precision=highest)
    carried_key = jnp.einsum('cshb,hcab->csha', value_blocks, after, precision=highest)
    carried_value = jnp.einsum('csha,hcab->cshb', key_blocks, after, precision=highest)
    grad_query = ((inner_query + grow * carried_query) / E).astype(jnp.bfloat16).reshape(length, width)
    grad_key = (inner_key / E + shrink * carried_key).astype(jnp.bfloat16).reshape(length, width)
    grad_value = (inner_value / E + shrink * carried_value).astype(jnp.bfloat16).reshape(length, width)
    return (grad_query, grad_key, grad_value)

def reference(mid, second_in, cotangent, w_key, w_value, w_query, w_out, w_ret_out, ret_query, ret_key, ret_value, gate, decay_exp, mask_start):
    keys = jnp.dot(mid, w_key, preferred_element_type=jnp.float32).astype(jnp.bfloat16)
    values = jnp.dot(mid, w_value, preferred_element_type=jnp.float32).astype(jnp.bfloat16)
    positions = jnp.arange(TOKENS, dtype=jnp.int32)
    first_seen = jnp.repeat(mask_start, BLK)
    visible = (positions[None, :] >= first_seen[:, None]) & (positions[None, :] <= positions[:, None])
    upper_in, upper_key, upper_value = attend_back(second_in, w_query[1], w_out[1], cotangent, keys, values, visible)
    upstream = (cotangent.astype(jnp.float32) + upper_in).astype(jnp.bfloat16)
    lower_in, lower_key, lower_value = attend_back(mid, w_query[0], w_out[0], upstream, keys, values, visible)
    key_grad = (upper_key + lower_key).astype(jnp.bfloat16)
    value_grad = (upper_value + lower_value).astype(jnp.bfloat16)
    grad_mid = (upstream.astype(jnp.float32) + lower_in + contract_last(key_grad, w_key) + contract_last(value_grad, w_value)).astype(jnp.bfloat16)
    tokens_dims = (((0,), (0,)), ((), ()))
    grad_w_key = lax.dot_general(mid, key_grad, tokens_dims, preferred_element_type=jnp.float32)
    grad_w_value = lax.dot_general(mid, value_grad, tokens_dims, preferred_element_type=jnp.float32)
    grad_o = contract_last(grad_mid, w_ret_out).astype(jnp.bfloat16)
    accum, ends, shrink, own_state = retention_states(ret_key, ret_value, gate, decay_exp)
    grow, own_grad = grad_states(ret_query, grad_o, accum)
    decays = jnp.exp(ends)
    zeros = jnp.zeros((gate.shape[0], E, E), jnp.float32)

    def forward(state, items):
        return (items[0][:, None, None] * state + items[1], state)

    def backward(state, items):
        return (items[1] + items[0][:, None, None] * state, state)
    unused_state, entering = lax.scan(forward, zeros, (decays.T, jnp.moveaxis(own_state, 1, 0)))
    unused_grad, after = lax.scan(backward, zeros, (decays.T, jnp.moveaxis(own_grad, 1, 0)), reverse=True)
    entering = jnp.moveaxis(entering, 0, 1)
    after = jnp.moveaxis(after, 0, 1)
    grad_query, grad_key, grad_value = retention_grads(ret_query, ret_key, ret_value, grad_o, accum, shrink, grow, entering, after)
    return (grad_mid, grad_query, grad_key, grad_value, grad_w_key, grad_w_value)
```

```python
import math

import jax
import jax.numpy as jnp
from jax import lax
from jax.experimental.layout import Layout, with_layout_constraint
from jax.sharding import PartitionSpec as P

E = 128
BLK = 128
RC = 128


def shifted(value, axis, step):
    peers = lax.axis_size(axis)
    return lax.ppermute(value, axis, [(i, (i + step) % peers) for i in range(peers)])


def swapped(value, axis):
    peers = lax.axis_size(axis)
    return lax.ppermute(value, axis, [(i, i ^ 1) for i in range(peers)])


def pair_sources(axis):
    peers, position = lax.axis_size(axis), lax.axis_index(axis)
    same = (position - 2 * jnp.arange(peers // 2, dtype=jnp.int32)) % peers
    return jnp.concatenate([same, same ^ 1])


def gather_pairs(value, axis):
    peers = lax.axis_size(axis)
    held = [value] + [shifted(value, axis, 2 * k) for k in range(1, peers // 2)]
    held = jnp.stack(held)
    return jnp.concatenate([held, swapped(held, axis)])


def scatter_pairs(parts, axis):
    half = lax.axis_size(axis) // 2
    crossing = swapped(parts[half:].astype(jnp.bfloat16), axis)
    joined = parts[:half] + crossing.astype(jnp.float32)
    total = joined[0]
    for k in range(1, half):
        total = total + shifted(joined[k].astype(jnp.bfloat16), axis, -2 * k).astype(jnp.float32)
    return total


def between(logs, low, high):
    places = jnp.arange(logs.shape[0], dtype=jnp.int32)
    inside = (places[None, :] > low[:, None]) & (places[None, :] < high[:, None])
    return jnp.sum(jnp.where(inside[:, :, None], logs[None], 0.0), axis=1)


def contract_last(left, right):
    return lax.dot_general(
        left, right, (((1,), (1,)), ((), ())), preferred_element_type=jnp.float32
    )


def attend_back(layer_in, w_query_l, w_out_l, upstream, keys, values, visible):
    row_count = layer_in.shape[0]
    key_count = keys.shape[0]
    kv_heads = keys.shape[1] // E
    factor = 1.0 / math.sqrt(E)
    queries = jnp.dot(layer_in, w_query_l, preferred_element_type=jnp.float32).astype(jnp.bfloat16)
    group = queries.shape[1] // keys.shape[1]
    grad_out = contract_last(upstream, w_out_l).astype(jnp.bfloat16)
    query_heads = queries.reshape(row_count, kv_heads, group, E)
    grad_heads = grad_out.reshape(row_count, kv_heads, group, E)
    key_heads = keys.reshape(key_count, kv_heads, E)
    value_heads = values.reshape(key_count, kv_heads, E)
    scores = (
        jnp.einsum("tkge,ske->kgts", query_heads, key_heads, preferred_element_type=jnp.float32)
        * factor
    )
    scores = jnp.where(visible, scores, -jnp.inf)
    top = jnp.max(scores, axis=-1, keepdims=True)
    raised = jnp.exp(scores - top)
    probs = raised / jnp.sum(raised, axis=-1, keepdims=True)
    rounded = probs.astype(jnp.bfloat16)
    outputs = jnp.einsum(
        "kgts,ske->tkge", rounded, value_heads, preferred_element_type=jnp.float32
    ).astype(jnp.bfloat16)
    delta = jnp.sum(grad_heads.astype(jnp.float32) * outputs.astype(jnp.float32), axis=-1)
    delta = jnp.transpose(delta, (1, 2, 0))[..., None]
    dprobs = jnp.einsum(
        "tkge,ske->kgts", grad_heads, value_heads, preferred_element_type=jnp.float32
    )
    dscores = (probs * (dprobs - delta) * factor).astype(jnp.bfloat16)
    query_grad = jnp.einsum(
        "kgts,ske->tkge", dscores, key_heads, preferred_element_type=jnp.float32
    )
    query_grad = query_grad.astype(jnp.bfloat16).reshape(row_count, -1)
    key_part = jnp.einsum(
        "kgts,tkge->ske", dscores, query_heads, preferred_element_type=jnp.float32
    ).reshape(key_count, -1)
    value_part = jnp.einsum(
        "kgts,tkge->ske", rounded, grad_heads, preferred_element_type=jnp.float32
    ).reshape(key_count, -1)
    return (contract_last(query_grad, w_query_l), key_part, value_part)


def retention_states(ret_key, ret_value, gate, decay_exp):
    length, width = ret_key.shape
    heads = gate.shape[0]
    size = width // heads
    count = length // RC
    key_blocks = ret_key.reshape(count, RC, heads, size)
    value_blocks = ret_value.reshape(count, RC, heads, size)
    rate = jnp.exp2(-decay_exp.astype(jnp.float32) / 64.0)
    steps = (-rate[:, None] * gate).reshape(heads * count, RC)
    upper = (jnp.arange(RC)[:, None] <= jnp.arange(RC)[None, :]).astype(jnp.float32)
    accum = jnp.dot(steps, upper, precision=lax.Precision.HIGHEST).reshape(heads, count, RC)
    ends = accum[:, :, -1]
    shrink = jnp.transpose(jnp.exp(ends[:, :, None] - accum), (1, 2, 0))[..., None]
    weighted = (shrink * key_blocks).astype(jnp.bfloat16)
    own_state = jnp.einsum(
        "csha,cshb->hcab", weighted, value_blocks, preferred_element_type=jnp.float32
    )
    return (accum, ends, shrink, own_state)


def grad_states(ret_query, grad_o, accum):
    heads, count, block = accum.shape
    size = ret_query.shape[1] // heads
    query_blocks = ret_query.reshape(count, block, heads, size)
    grad_blocks = grad_o.reshape(count, block, heads, size)
    grow = jnp.transpose(jnp.exp(accum), (1, 2, 0))[..., None]
    weighted = (grow * query_blocks).astype(jnp.bfloat16)
    own_grad = (
        jnp.einsum("ctha,cthb->hcab", weighted, grad_blocks, preferred_element_type=jnp.float32) / E
    )
    return (grow, own_grad)


def retention_grads(ret_query, ret_key, ret_value, grad_o, accum, shrink, grow, entering, after):
    length, width = ret_query.shape
    heads, count, block = accum.shape
    size = width // heads
    shape4 = (count, block, heads, size)
    query_blocks = ret_query.reshape(shape4)
    key_blocks = ret_key.reshape(shape4)
    value_blocks = ret_value.reshape(shape4)
    grad_blocks = grad_o.reshape(shape4)
    lower = jnp.arange(block)[:, None] >= jnp.arange(block)[None, :]
    diff = accum[:, :, :, None] - accum[:, :, None, :]
    weights = jnp.where(lower, jnp.exp(jnp.where(lower, diff, 0.0)), 0.0)
    first = (
        weights
        * jnp.einsum(
            "ctha,csha->hcts", grad_blocks, value_blocks, preferred_element_type=jnp.float32
        )
    ).astype(jnp.bfloat16)
    second = (
        weights
        * jnp.einsum(
            "ctha,csha->hcts", query_blocks, key_blocks, preferred_element_type=jnp.float32
        )
    ).astype(jnp.bfloat16)
    inner_query = jnp.einsum(
        "hcts,csha->ctha", first, key_blocks, preferred_element_type=jnp.float32
    )
    inner_key = jnp.einsum(
        "hcts,ctha->csha", first, query_blocks, preferred_element_type=jnp.float32
    )
    inner_value = jnp.einsum(
        "hcts,ctha->csha", second, grad_blocks, preferred_element_type=jnp.float32
    )
    highest = lax.Precision.HIGHEST
    carried_query = jnp.einsum(
        "cthb,hcab->ctha", grad_blocks.astype(jnp.float32), entering, precision=highest
    )
    carried_key = jnp.einsum(
        "cshb,hcab->csha", value_blocks.astype(jnp.float32), after, precision=highest
    )
    carried_value = jnp.einsum(
        "csha,hcab->cshb", key_blocks.astype(jnp.float32), after, precision=highest
    )
    grad_query = (
        ((inner_query + grow * carried_query) / E).astype(jnp.bfloat16).reshape(length, width)
    )
    grad_key = (inner_key / E + shrink * carried_key).astype(jnp.bfloat16).reshape(length, width)
    grad_value = (
        (inner_value / E + shrink * carried_value).astype(jnp.bfloat16).reshape(length, width)
    )
    return (grad_query, grad_key, grad_value)


def head_total(partial_value, residual):
    peers, position = lax.axis_size("head"), lax.axis_index("head")
    piece = partial_value.shape[0] // peers

    def rows_of(array, owner):
        return lax.dynamic_slice_in_dim(array, owner * piece, piece, 0).astype(jnp.float32)

    sent = partial_value.astype(jnp.bfloat16)
    total = rows_of(residual, position) + rows_of(sent, position)
    for k in range(1, peers):
        out = rows_of(sent, (position + k) % peers).astype(jnp.bfloat16)
        total = total + shifted(out, "head", k).astype(jnp.float32)
    mine = total.astype(jnp.bfloat16)
    whole = jnp.zeros_like(residual)
    whole = lax.dynamic_update_slice_in_dim(whole, mine, position * piece, 0)
    for k in range(1, peers):
        got = shifted(mine, "head", k)
        whole = lax.dynamic_update_slice_in_dim(whole, got, ((position - k) % peers) * piece, 0)
    return whole


def local(
    mid,
    second_in,
    cotangent,
    w_key,
    w_value,
    w_query,
    w_out,
    w_ret_out,
    ret_query,
    ret_key,
    ret_value,
    gate,
    decay_exp,
    mask_start,
):
    row_count = mid.shape[0]
    position = lax.axis_index("seq")
    keys_own = jnp.dot(mid, w_key, preferred_element_type=jnp.float32).astype(jnp.bfloat16)
    values_own = jnp.dot(mid, w_value, preferred_element_type=jnp.float32).astype(jnp.bfloat16)
    width_own = keys_own.shape[1]
    pairs = gather_pairs(jnp.concatenate([keys_own, values_own], axis=1), "seq")
    sources = pair_sources("seq")
    all_keys = pairs[:, :, :width_own].reshape(-1, width_own)
    all_values = pairs[:, :, width_own:].reshape(-1, width_own)
    key_count = all_keys.shape[0]
    positions = lax.axis_index("seq") * row_count + jnp.arange(row_count, dtype=jnp.int32)
    first_seen = jnp.repeat(mask_start, BLK)
    key_positions = sources[:, None] * row_count + jnp.arange(row_count, dtype=jnp.int32)[None, :]
    key_positions = key_positions.reshape(key_count)
    visible = (key_positions[None, :] >= first_seen[:, None]) & (
        key_positions[None, :] <= positions[:, None]
    )
    upper_in, upper_key, upper_value = attend_back(
        second_in, w_query[1], w_out[1], cotangent, all_keys, all_values, visible
    )
    upper_in, ret_key, ret_value, gate = lax.optimization_barrier(
        (upper_in.astype(jnp.bfloat16), ret_key, ret_value, gate)
    )
    accum, ends, shrink, own_state = retention_states(ret_key, ret_value, gate, decay_exp)
    decay_rows = jnp.exp(ends)
    count = decay_rows.shape[1]
    device_log = jnp.sum(ends, axis=1)
    device_state = jnp.zeros_like(own_state[:, 0])
    for block in range(count):
        device_state = decay_rows[:, block, None, None] * device_state + own_state[:, block]
    log_high = lax.reduce_precision(device_log, 8, 7)
    log_middle = lax.reduce_precision(device_log - log_high, 8, 7)
    log_low = device_log - log_high - log_middle
    logs = jnp.stack([log_high, log_middle, log_low], axis=1)
    logs = jnp.pad(logs, ((0, 0), (0, 13)))[:, :, None]
    logs = jnp.broadcast_to(logs, logs.shape[:2] + (device_state.shape[2],))
    packed = jnp.concatenate([device_state, logs], axis=1).astype(jnp.bfloat16)
    states = lax.all_gather(packed, "seq")
    upstream = head_total(upper_in, cotangent)
    lower_in, lower_key, lower_value = attend_back(
        mid, w_query[0], w_out[0], upstream, all_keys, all_values, visible
    )
    parts = jnp.concatenate([upper_key + lower_key, upper_value + lower_value], axis=1)
    parts, states = lax.optimization_barrier((parts, states))
    totals = scatter_pairs(parts.reshape(pairs.shape), "seq").astype(jnp.bfloat16)
    size = device_state.shape[1]
    all_logs = jnp.sum(states[:, :, size : size + 3, 0].astype(jnp.float32), axis=2)
    places = jnp.arange(states.shape[0], dtype=jnp.int32)
    here = jnp.full_like(places, position)
    share = jnp.where((places < position)[:, None], jnp.exp(between(all_logs, places, here)), 0.0)
    incoming = jnp.sum(share[:, :, None, None] * states[:, :, :size].astype(jnp.float32), axis=0)
    key_grad, value_grad = totals[:, :width_own], totals[:, width_own:]
    tokens_dims = (((0,), (0,)), ((), ()))
    weight_parts = tuple(
        with_layout_constraint(
            lax.dot_general(
                mid, half, tokens_dims, preferred_element_type=jnp.float32
            ).astype(jnp.bfloat16),
            Layout((0, 1)),
        )
        for half in (key_grad, value_grad)
    )
    mid_part = lower_in + contract_last(key_grad, w_key) + contract_last(value_grad, w_value)
    mid_part, weight_parts = lax.optimization_barrier(
        (mid_part.astype(jnp.bfloat16), weight_parts)
    )
    weight_sums = lax.psum(weight_parts, "seq")
    grad_w_key, grad_w_value = (part.astype(jnp.float32) for part in weight_sums)
    grad_mid = head_total(mid_part, upstream)
    grad_o = contract_last(grad_mid, w_ret_out).astype(jnp.bfloat16)
    grow, own_grad = grad_states(ret_query, grad_o, accum)
    device_grad = jnp.zeros_like(device_state)
    for block in reversed(range(count)):
        device_grad = own_grad[:, block] + decay_rows[:, block, None, None] * device_grad
    after_states = gather_pairs(device_grad.astype(jnp.bfloat16), "seq")
    here = jnp.full_like(sources, position)
    share = jnp.where((sources > position)[:, None], jnp.exp(between(all_logs, here, sources)), 0.0)
    outgoing = jnp.sum(share[:, :, None, None] * after_states.astype(jnp.float32), axis=0)
    entering_list = []
    state_now = incoming
    for block in range(count):
        entering_list.append(state_now)
        state_now = decay_rows[:, block, None, None] * state_now + own_state[:, block]
    after_list = [state_now] * count
    state_now = outgoing
    for block in reversed(range(count)):
        after_list[block] = state_now
        state_now = own_grad[:, block] + decay_rows[:, block, None, None] * state_now
    entering = jnp.stack(entering_list, axis=1)
    after = jnp.stack(after_list, axis=1)
    grad_query, grad_key, grad_value = retention_grads(
        ret_query, ret_key, ret_value, grad_o, accum, shrink, grow, entering, after
    )
    return (grad_mid, grad_query, grad_key, grad_value, grad_w_key, grad_w_value)


def solution(mesh):
    placed = (
        P("seq", None),
        P("seq", None),
        P("seq", None),
        P(None, "head"),
        P(None, "head"),
        P(None, None, "head"),
        P(None, "head", None),
        P("head", None),
        P("seq", "head"),
        P("seq", "head"),
        P("seq", "head"),
        P("head", "seq"),
        P("head"),
        P("seq"),
    )
    return jax.shard_map(
        local,
        mesh=mesh,
        in_specs=placed,
        out_specs=(
            P("seq", None),
            P("seq", "head"),
            P("seq", "head"),
            P("seq", "head"),
            P(None, "head"),
            P(None, "head"),
        ),
        check_vma=False,
    )
```
